32 devices in a mesh: seq: 8 (over z, x), head: 4 (over y, core).
Axes of the slice: x: 2, y: 2, z: 4, core: 2. Of those that a mesh axis runs over, the one named last changes fastest.
Arguments:
- queries: bfloat16 [4096, 1024], P('seq', 'head'), may hold values from -6 to 6
- key_vectors: bfloat16 [4096, 1024], P('seq', 'head'), may hold values from -6 to 6
- values: bfloat16 [4096, 2048], P('seq', 'head'), may hold values from -6 to 6
- log_gate: bfloat16 [4096, 1024], P('seq', 'head'), may hold values from -1.6 to 0, as said below
- out_gate: bfloat16 [4096, 2048], P('seq', 'head'), may hold values from -6 to 6
- norm_gain: float32 [2048], P('head'), may hold values from 0.5 to 1.5
- out_weight: bfloat16 [2048, 2048], P('head'), may hold values from -0.1875 to 0.1875
Outputs:
- mixed: bfloat16 [4096, 2048], P('seq', 'head')
The draws below stay inside these ranges and needn't reach their ends.
Inputs may be any that keep to these rules, and one draw needn't show every extreme that they name: `log_gate`: every entry is below zero.
All inputs are finite; a program needn't handle non-finite values.
Results may differ from the reference program's by a relative error of at most 0.017.
Values may be sent and summed in bfloat16 or wider, within the bound.
A program may use at most 128 MiB of HBM per device.

```python
import jax
import jax.numpy as jnp
from jax import lax

D = 2048
H = 4
DK = 256
DV = 512
SPAN = 64
TOK_DEV = 512
SEQUENCE_TOKENS = 4096
N_HEAD = 4


def draw_log_gate(key, part):
    parallel_lanes = jax.random.split(key, 7)
    blocks_all = SEQUENCE_TOKENS // TOK_DEV
    quick_count = H // 2
    order = jax.random.permutation(parallel_lanes[0], H)
    quick_head = order < quick_count
    quick_rate = jnp.exp(jax.random.uniform(parallel_lanes[1], (H, DK), minval=jnp.log(0.02), maxval=jnp.log(0.06)))
    slow_rate = jnp.exp(jax.random.uniform(parallel_lanes[2], (H, DK), minval=jnp.log(0.05), maxval=jnp.log(0.25))) / SEQUENCE_TOKENS
    base_rate = jnp.where(quick_head[:, None], quick_rate, slow_rate).reshape(1, 1, H * DK)
    device_factor = jnp.exp(jax.random.uniform(parallel_lanes[3], (blocks_all, 1, H * DK), minval=jnp.log(0.5), maxval=jnp.log(2.0)))
    roughness = jax.random.uniform(parallel_lanes[4], (blocks_all, TOK_DEV, H * DK), minval=0.5, maxval=1.5)
    decay_factor = (base_rate * device_factor * roughness).reshape(SEQUENCE_TOKENS, H * DK)
    block_offset = jax.random.randint(parallel_lanes[5], (2,), 0, SEQUENCE_TOKENS)
    block_length = jnp.log(jax.random.uniform(parallel_lanes[6], (2,), minval=0.5, maxval=0.8))
    token_position = lax.iota(jnp.int32, SEQUENCE_TOKENS)
    token_block = jnp.sum(jnp.where(token_position[:, None] == block_offset[None, :], block_length[None, :], 0.0), axis=1)
    return (token_block[:, None] - decay_factor).astype(jnp.bfloat16)


def raised(entries, rng, source, target, parts, factor):
    def block_of(dim):
        return (jnp.arange(entries.shape[dim]) // (entries.shape[dim] // parts)).reshape((-1,) + (1,) * (entries.ndim - 1 - dim))

    near = jax.random.permutation(rng, parts)[block_of(target)]
    other_side = (block_of(target) + parts // 2) % parts
    return jnp.where((block_of(source) == near) | (block_of(source) == other_side), factor * entries, entries)


def steps_of(stream_key, dims, pieces, least, largest):
    def one(axis_at, shards_of):
        heights = jax.random.uniform(jax.random.fold_in(jax.random.fold_in(stream_key, 6), axis_at), (shards_of,), jnp.float32, least / len(pieces), largest / len(pieces))
        return jnp.repeat(jnp.exp(heights), dims[axis_at] // shards_of).reshape((-1,) + (1,) * (len(dims) - axis_at - 1))

    factor_of = one(*pieces[0])
    for cut in pieces[1:]:
        factor_of = factor_of * one(*cut)
    return factor_of


def normal_values(stream_key, shape, scale, most, cuts=(), kind=jnp.bfloat16):
    factor_of = steps_of(stream_key, shape, cuts, -0.22, 0.18) if cuts else 1.0
    result = jax.random.normal(stream_key, shape, jnp.float32) * scale * factor_of
    return jnp.minimum(jnp.maximum(result, -most), most).astype(kind)


def noise_with(own_key, dims, scale, reach, cuts, heavy, dtype=jnp.bfloat16):
    array = scale * jax.random.normal(own_key, dims, jnp.float32)
    if cuts:
        array = array * steps_of(own_key, dims, cuts, -0.22, 0.18)
    return jnp.clip(raised(array, jax.random.fold_in(own_key, 3), *heavy), -reach, reach).astype(dtype)


def setup_inputs(seed: int = 0) -> dict:
    streams_of = jax.random.split(jax.random.key(seed), 8)
    queries = normal_values(streams_of[0], (SEQUENCE_TOKENS, H * DK), 1.0, 6.0, ((0, 8), (1, 4)))
    key_vectors = normal_values(streams_of[1], (SEQUENCE_TOKENS, H * DK), 1.0, 6.0, ((0, 8), (1, 4)))
    values = normal_values(streams_of[2], (SEQUENCE_TOKENS, H * DV), 1.0, 6.0, ((0, 8), (1, 4)))
    log_gate = draw_log_gate(jax.random.fold_in(streams_of[7], 71), 0)
    out_gate = normal_values(streams_of[4], (SEQUENCE_TOKENS, H * DV), 1.0, 6.0, ((0, 8), (1, 4)))
    norm_gain = jnp.clip(1.0 + 0.1 * jax.random.normal(streams_of[5], (H * DV,), jnp.float32), 0.5, 1.5)
    out_weight = noise_with(streams_of[6], (H * DV, D), (H * DV) ** -0.5, 0.1875, ((0, 4),), (0, 1, 4, 2.0))
    return {"queries": queries, "key_vectors": key_vectors, "values": values, "log_gate": log_gate, "out_gate": out_gate, "norm_gain": norm_gain, "out_weight": out_weight}


def lowered(array_in):
    return lax.optimization_barrier(array_in.astype(jnp.bfloat16)).astype(jnp.float32)

def reference(queries, key_vectors, values, log_gate, out_gate, norm_gain, out_weight):
    blocks = SEQUENCE_TOKENS // SPAN
    middle_pos = SPAN // 2
    causal = lax.iota(jnp.int32, SPAN)[:, None] >= lax.iota(jnp.int32, SPAN)[None, :]
    gain_table = norm_gain.reshape(H, DV)

    def advance(carried, block_in):
        query_b, key_b, value_b, gate_b, outer_b = block_in
        running = jnp.cumsum(gate_b.astype(jnp.float32), axis=0)
        middle = running[middle_pos:middle_pos + 1]
        ending = running[SPAN - 1:SPAN]
        query_f = query_b.astype(jnp.float32)
        key_f = key_b.astype(jnp.float32)
        value_f = value_b.astype(jnp.float32)
        q_inter = lowered(query_f * jnp.exp(running))
        q_intra = lowered(query_f * jnp.exp(running - middle))
        k_intra = lowered(key_f * jnp.exp(middle - running))
        k_state = lowered(key_f * jnp.exp(ending - running))
        scores = jnp.einsum('thd,shd->hts', q_intra, k_intra)
        weights = lowered(jnp.where(causal[None], scores, 0.0))
        local_part = jnp.einsum('hts,she->the', weights, value_f)
        carried_low = lowered(carried)
        carried_part = jnp.einsum('thd,hed->the', q_inter, carried_low)
        attention = local_part + carried_part
        spread = lax.optimization_barrier(jnp.mean(attention * attention, axis=-1, keepdims=True))
        normed = attention / jnp.sqrt(spread + 1e-05) * gain_table
        gated_out = (normed * jax.nn.silu(outer_b.astype(jnp.float32))).astype(jnp.bfloat16)
        block_state = jnp.einsum('the,thd->hed', value_f, k_state)
        carried = carried * jnp.exp(ending[0])[:, None, :] + block_state
        return (carried, gated_out.reshape(SPAN, H * DV))
    start_state = jnp.zeros((H, DV, DK), jnp.float32)
    inputs = (queries.reshape(blocks, SPAN, H, DK), key_vectors.reshape(blocks, SPAN, H, DK), values.reshape(blocks, SPAN, H, DV), log_gate.reshape(blocks, SPAN, H, DK), out_gate.reshape(blocks, SPAN, H, DV))
    unused_state, gated_all = lax.scan(advance, start_state, inputs)
    gated_all = gated_all.reshape(SEQUENCE_TOKENS, H * DV)
    group_width = H // N_HEAD * DV
    summed = jnp.zeros((SEQUENCE_TOKENS, D), jnp.float32)
    for group_index in range(N_HEAD):
        start_row = group_index * group_width
        end_row = start_row + group_width
        partial_value = jnp.dot(gated_all[:, start_row:end_row], out_weight[start_row:end_row], preferred_element_type=jnp.float32)
        summed = summed + lowered(partial_value)
    return summed.astype(jnp.bfloat16)
```

```python
import functools

import jax
import jax.numpy as jnp
from jax import lax
from jax.experimental import pallas as pl
from jax.experimental.pallas import tpu as pltpu
from jax.sharding import PartitionSpec as P

DK = 256
DV = 512
SPAN = 64
CHUNKS = 4
TOKENS = 128
F32 = jnp.float32
BF16 = jnp.bfloat16
MESH = pl.DeviceIdType.MESH


def dot(a, b, dims=((1,), (0,))):
    return lax.dot_general(a, b, (dims, ((), ())), preferred_element_type=F32)


def kernel(
    n_seq, n_head,
    q_hbm, k_hbm, v_hbm, g_hbm, o_hbm, gain_hbm, w_hbm,
    out_hbm,
    q, k, v, g, o, gain, w,
    run, ends, kd, qg, att, act, state,
    log_out, log_in, half_out, half_in, own_half, chain_out, chain_in, pass_out, carry,
    gated, mine, y_out, y_in, out,
    load_sem, w_sem, w_send, w_recv, log_sem, half_send, half_recv,
    chain_send, chain_recv, pass_send, pass_recv, g_send, g_recv, y_send, y_recv, out_sem,
):
    length = q.shape[0]
    blocks = length // SPAN
    pieces = length // TOKENS
    groups = n_head // 2
    width = w_hbm.shape[1] // n_head
    half = DV // 2
    rows = half // CHUNKS
    seq = lax.axis_index("seq")
    head = lax.axis_index("head")
    x = lax.rem(seq, 2)
    z = lax.div(seq, 2)
    last = n_seq // 2 - 1
    core = lax.rem(head, 2)
    group = lax.div(head, 2)
    across = {"seq": seq + 1 - 2 * x, "head": head}
    onward = {"seq": lax.rem(seq + 2, n_seq), "head": head}
    back = {"seq": lax.rem(seq + n_seq - 2, n_seq), "head": head}
    partner = {"seq": seq, "head": head + 1 - 2 * core}
    peers = [
        {"seq": seq, "head": lax.rem(head + 2 * step, n_head)} for step in range(1, groups)
    ]

    def columns(which_group, which_core):
        return pl.ds(pl.multiple_of((which_group * 2 + which_core) * width, 128), width)

    loads = [
        pltpu.make_async_copy(src, dst, load_sem.at[i])
        for i, (src, dst) in enumerate(
            ((g_hbm, g), (k_hbm, k), (v_hbm, v), (q_hbm, q), (o_hbm, o), (gain_hbm, gain))
        )
    ]
    for load in loads:
        load.start()
    w_loads = [
        pltpu.make_async_copy(
            w_hbm.at[:, columns(lax.rem(group + j, groups), core)], w.at[0, j], w_sem.at[j]
        )
        for j in range(groups)
    ]
    barrier = pltpu.get_barrier_semaphore()
    friends = [across, onward, back, partner] + peers
    for friend in friends:
        pl.semaphore_signal(barrier, inc=1, device_id=friend, device_id_type=MESH)

    def remote(src, dst, send, recv, device):
        return pltpu.make_async_remote_copy(
            src_ref=src, dst_ref=dst, send_sem=send, recv_sem=recv,
            device_id=device, device_id_type=MESH,
        )

    @pl.when(z == 0)
    def _():
        chain_in[...] = jnp.zeros_like(chain_in)

    tri = (
        lax.broadcasted_iota(jnp.int32, (SPAN, SPAN), 0)
        >= lax.broadcasted_iota(jnp.int32, (SPAN, SPAN), 1)
    )
    ones = jnp.where(tri, 1.0, 0.0).astype(BF16)
    loads[0].wait()
    total = jnp.zeros((1, DK), F32)
    endings = []
    for b in range(blocks):
        r = dot(ones, g[b * SPAN : (b + 1) * SPAN, :])
        run[b] = r
        endings.append(r[SPAN - 1 : SPAN, :])
        ends[b : b + 1, :] = total
        total = total + endings[b]
    log_out[...] = jnp.broadcast_to(total, log_out.shape)
    loads[1].wait()
    tail = jnp.zeros((1, DK), F32)
    for b in reversed(range(blocks)):
        part = slice(b * SPAN, (b + 1) * SPAN)
        kd[part, :] = (k[part, :].astype(F32) * jnp.exp((endings[b] - run[b]) + tail)).astype(BF16)
        tail = tail + endings[b]

    pl.semaphore_wait(barrier, len(friends))
    log_copy = remote(log_out, log_in, log_sem.at[0], log_sem.at[1], across)
    log_copy.start()
    loads[2].wait()

    def half_state(which):
        cols = pl.ds(pl.multiple_of(which * half, 128), half)
        return dot(v[:, cols], kd[...], ((0,), (0,)))

    theirs = half_state(1 - x).astype(BF16)
    half_copies = []
    for i in range(CHUNKS):
        half_out[i] = theirs[i * rows : (i + 1) * rows, :]
        copy = remote(half_out.at[i], half_in.at[i], half_send.at[i], half_recv.at[i], across)
        copy.start()
        half_copies.append(copy)
    own_half[...] = half_state(x).reshape(CHUNKS, rows, DK)
    for load in w_loads:
        load.start()
    w_copies = [
        remote(
            w_hbm.at[:, columns(lax.rem(group + j, groups), 1 - core)], w.at[1, j],
            w_send.at[j], w_recv.at[j], partner,
        )
        for j in range(groups)
    ]
    for copy in w_copies:
        copy.start()

    for load in loads[3:]:
        load.wait()
    state[...] = jnp.zeros_like(state)

    def local(b, _):
        part = pl.ds(pl.multiple_of(b * SPAN, SPAN), SPAN)
        r = run[b]
        middle = r[SPAN // 2 : SPAN // 2 + 1, :]
        ending = r[SPAN - 1 : SPAN, :]
        before = ends[pl.ds(b, 1), :]
        qf = q[part, :].astype(F32)
        kf = k[part, :].astype(F32)
        qi = qf * jnp.exp(r)
        qg[part, :] = (qi * jnp.exp(before)).astype(BF16)
        q_intra = (qf * jnp.exp(r - middle)).astype(BF16)
        k_intra = (kf * jnp.exp(middle - r)).astype(BF16)
        k_state = (kf * jnp.exp(ending - r)).astype(BF16)
        vb = v[part, :]
        scores = dot(q_intra, k_intra, ((1,), (1,)))
        weights = jnp.where(tri, scores, 0.0).astype(BF16)
        held = state[...]
        att[part, :] = dot(weights, vb) + dot(qi.astype(BF16), held.astype(BF16), ((1,), (1,)))
        state[...] = held * jnp.exp(ending) + dot(vb, k_state, ((0,), (0,)))
        of = o[part, :].astype(F32)
        act[part, :] = of / (1.0 + jnp.exp(-of)) * gain[...]
        return 0

    lax.fori_loop(0, blocks, local, 0)

    log_copy.wait()
    mine_log = log_out[0:1, :]
    their_log = log_in[0:1, :]
    first = x == 0
    decay0 = jnp.exp(jnp.where(first, mine_log, their_log))
    decay1 = jnp.exp(jnp.where(first, their_log, mine_log))
    chain_copies = []
    pass_copies = []
    for i in range(CHUNKS):
        half_copies[i].wait_recv()
        chain = remote(
            chain_out.at[i], chain_in.at[i], chain_send.at[i], chain_recv.at[i], onward
        )
        chain_copies.append(chain)
        own = own_half[i]
        other = half_in[i].astype(F32)
        s0 = jnp.where(first, own, other)
        s1 = jnp.where(first, other, own)

        @pl.when(z > 0)
        def _():
            chain.wait_recv()

        entering = chain_in[i].astype(F32)
        between = decay0 * entering + s0
        chain_out[i] = (decay1 * between + s1).astype(BF16)

        @pl.when(z < last)
        def _():
            chain.start()

        pass_out[i] = jnp.where(first, between, entering).astype(BF16)
        carry[x, i] = jnp.where(first, entering, between).astype(BF16)
        passing = remote(
            pass_out.at[i], carry.at[x, i], pass_send.at[i], pass_recv.at[i], across
        )
        passing.start()
        pass_copies.append(passing)
    for passing in pass_copies:
        passing.wait_recv()
    carried = carry[...].reshape(DV, DK)

    g_copies = []
    for i in range(pieces):
        part = slice(i * TOKENS, (i + 1) * TOKENS)
        a = att[part, :] + dot(qg[part, :], carried, ((1,), (1,)))
        spread = jnp.mean(a * a, axis=-1, keepdims=True)
        gated[0, part, :] = (a * lax.rsqrt(spread + 1e-05) * act[part, :]).astype(BF16)
        copy = remote(
            gated.at[0, part, :], gated.at[1, part, :], g_send.at[i], g_recv.at[i], partner
        )
        copy.start()
        g_copies.append(copy)
    for copy in w_loads:
        copy.wait()
    for copy in w_copies:
        copy.wait_recv()
    y_copies = []
    for i in range(pieces):
        part = slice(i * TOKENS, (i + 1) * TOKENS)
        g_copies[i].wait_recv()
        for j in range(1, groups):
            y_out[j - 1, part, :] = (
                dot(gated[0, part, :], w[0, j]) + dot(gated[1, part, :], w[1, j])
            ).astype(BF16)
            copy = remote(
                y_out.at[j - 1, part, :], y_in.at[j - 1, part, :],
                y_send.at[j - 1, i], y_recv.at[j - 1, i], peers[j - 1],
            )
            copy.start()
            y_copies.append(copy)
    for i in range(pieces):
        part = slice(i * TOKENS, (i + 1) * TOKENS)
        mine[part, :] = dot(gated[0, part, :], w[0, 0]) + dot(gated[1, part, :], w[1, 0])
    stores = []
    for i in range(pieces):
        part = slice(i * TOKENS, (i + 1) * TOKENS)
        total_out = mine[part, :]
        for j in range(1, groups):
            y_copies[i * (groups - 1) + j - 1].wait_recv()
            total_out = total_out + y_in[j - 1, part, :].astype(F32)
        out[part, :] = total_out.astype(BF16)
        store = pltpu.make_async_copy(out.at[part, :], out_hbm.at[part, :], out_sem.at[i])
        store.start()
        stores.append(store)
    for copy in half_copies + pass_copies + w_copies + g_copies + y_copies:
        copy.wait_send()

    @pl.when(z < last)
    def _():
        for chain in chain_copies:
            chain.wait_send()

    for store in stores:
        store.wait()


def shards(n_seq, n_head, queries, key_vectors, values, log_gate, out_gate, norm_gain, out_weight):
    length = queries.shape[0]
    width = out_weight.shape[1] // n_head
    groups = n_head // 2
    blocks = length // SPAN
    pieces = length // TOKENS
    half_rows = DV // 2 // CHUNKS
    VM = pltpu.VMEM
    dma = pltpu.SemaphoreType.DMA
    piece_state = (CHUNKS, half_rows, DK)
    scratch = [
        VM((length, DK), BF16), VM((length, DK), BF16), VM((length, DV), BF16),
        VM((length, DK), BF16), VM((length, DV), BF16), VM((1, DV), F32),
        VM((2, groups, DV, width), BF16),
        VM((blocks, SPAN, DK), F32), VM((blocks, DK), F32), VM((length, DK), BF16),
        VM((length, DK), BF16), VM((length, DV), F32), VM((length, DV), F32), VM((DV, DK), F32),
        VM((8, DK), F32), VM((8, DK), F32), VM(piece_state, BF16), VM(piece_state, BF16),
        VM(piece_state, F32), VM(piece_state, BF16), VM(piece_state, BF16),
        VM(piece_state, BF16), VM((2,) + piece_state, BF16),
        VM((2, length, DV), BF16), VM((length, width), F32),
        VM((groups - 1, length, width), BF16), VM((groups - 1, length, width), BF16),
        VM((length, width), BF16),
        dma((6,)), dma((groups,)), dma((groups,)), dma((groups,)), dma((2,)),
        dma((CHUNKS,)), dma((CHUNKS,)), dma((CHUNKS,)), dma((CHUNKS,)),
        dma((CHUNKS,)), dma((CHUNKS,)), dma((pieces,)), dma((pieces,)),
        dma((groups - 1, pieces)), dma((groups - 1, pieces)), dma((pieces,)),
    ]
    return pl.pallas_call(
        functools.partial(kernel, n_seq, n_head),
        out_shape=jax.ShapeDtypeStruct((length, width), BF16),
        in_specs=[pl.BlockSpec(memory_space=pl.ANY)] * 7,
        out_specs=pl.BlockSpec(memory_space=pl.ANY),
        scratch_shapes=scratch,
        compiler_params=pltpu.CompilerParams(
            collective_id=0, has_side_effects=True, vmem_limit_bytes=56 * 2**20
        ),
        name="gated_layer",
    )(queries, key_vectors, values, log_gate, out_gate, norm_gain.reshape(1, DV), out_weight)


def solution(mesh):
    in_specs = (
        P("seq", "head"),
        P("seq", "head"),
        P("seq", "head"),
        P("seq", "head"),
        P("seq", "head"),
        P("head"),
        P("head", None),
    )
    out_specs = P("seq", "head")
    body = functools.partial(shards, mesh.shape["seq"], mesh.shape["head"])
    return jax.shard_map(body, mesh=mesh, in_specs=in_specs, out_specs=out_specs, check_vma=False)
```

```python
import functools

import jax
import jax.numpy as jnp
from jax import lax
from jax.experimental import pallas as pl
from jax.experimental.pallas import tpu as pltpu
from jax.sharding import PartitionSpec as P

DK = 256
DV = 512
SPAN = 64
CHUNKS = 8
TOKENS = 64
F32 = jnp.float32
BF16 = jnp.bfloat16
MESH = pl.DeviceIdType.MESH


def dot(a, b, dims=((1,), (0,))):
    return lax.dot_general(a, b, (dims, ((), ())), preferred_element_type=F32)


def kernel(
    n_seq, n_head,
    q_hbm, k_hbm, v_hbm, g_hbm, o_hbm, gain_hbm, w_hbm,
    out,
    q, k, v, g, o, gain, w,
    run, ends, kd, qg, att, act, state,
    log_out, log_in, half_out, half_in, own_half, chain_out, chain_in, pass_out, carry,
    gated, mine, y_out, y_in,
    load_sem, w_sem, w_send, w_recv, log_sem, half_send, half_recv,
    chain_send, chain_recv, pass_send, pass_recv, g_send, g_recv, y_send, y_recv,
):
    length = q.shape[0]
    blocks = length // SPAN
    pieces = length // TOKENS
    groups = n_head // 2
    width = w_hbm.shape[1] // n_head
    half = DV // 2
    rows = half // CHUNKS
    seq = lax.axis_index("seq")
    head = lax.axis_index("head")
    x = lax.rem(seq, 2)
    z = lax.div(seq, 2)
    last = n_seq // 2 - 1
    core = lax.rem(head, 2)
    group = lax.div(head, 2)
    across = {"seq": seq + 1 - 2 * x, "head": head}
    onward = {"seq": lax.rem(seq + 2, n_seq), "head": head}
    back = {"seq": lax.rem(seq + n_seq - 2, n_seq), "head": head}
    leads = z < last
    follows = z > 0
    partner = {"seq": seq, "head": head + 1 - 2 * core}
    peers = [
        {"seq": seq, "head": lax.rem(head + 2 * step, n_head)} for step in range(1, groups)
    ]

    def columns(which_group, which_core):
        return pl.ds(pl.multiple_of((which_group * 2 + which_core) * width, 128), width)

    loads = [
        pltpu.make_async_copy(src, dst, load_sem.at[i])
        for i, (src, dst) in enumerate(
            ((g_hbm, g), (k_hbm, k), (v_hbm, v), (q_hbm, q), (o_hbm, o), (gain_hbm, gain))
        )
    ]
    for load in loads:
        load.start()
    w_loads = [
        pltpu.make_async_copy(
            w_hbm.at[:, columns(lax.rem(group + j, groups), core)], w.at[0, j], w_sem.at[j]
        )
        for j in range(groups)
    ]
    barrier = pltpu.get_barrier_semaphore()

    def greet(friend):
        pl.semaphore_signal(barrier, inc=1, device_id=friend, device_id_type=MESH)

    for friend in [across, partner] + peers:
        greet(friend)
    pl.when(leads)(lambda: greet(onward))
    pl.when(follows)(lambda: greet(back))
    met = 2 + len(peers) + leads.astype(jnp.int32) + follows.astype(jnp.int32)

    def remote(src, dst, send, recv, device):
        return pltpu.make_async_remote_copy(
            src_ref=src, dst_ref=dst, send_sem=send, recv_sem=recv,
            device_id=device, device_id_type=MESH,
        )

    @pl.when(z == 0)
    def _():
        chain_in[...] = jnp.zeros_like(chain_in)

    tri = (
        lax.broadcasted_iota(jnp.int32, (SPAN, SPAN), 0)
        >= lax.broadcasted_iota(jnp.int32, (SPAN, SPAN), 1)
    )
    ones = jnp.where(tri, 1.0, 0.0).astype(BF16)
    loads[0].wait()
    total = jnp.zeros((1, DK), F32)
    endings = []
    for b in range(blocks):
        r = dot(ones, g[b * SPAN : (b + 1) * SPAN, :])
        run[b] = r
        endings.append(r[SPAN - 1 : SPAN, :])
        ends[b : b + 1, :] = total
        total = total + endings[b]
    log_out[...] = jnp.broadcast_to(total, log_out.shape)
    loads[1].wait()
    tail = jnp.zeros((1, DK), F32)
    for b in reversed(range(blocks)):
        part = slice(b * SPAN, (b + 1) * SPAN)
        kd[part, :] = (k[part, :].astype(F32) * jnp.exp((endings[b] - run[b]) + tail)).astype(BF16)
        tail = tail + endings[b]

    pl.semaphore_wait(barrier, met)
    log_copy = remote(log_out, log_in, log_sem.at[0], log_sem.at[1], across)
    log_copy.start()
    loads[2].wait()

    def half_state(which):
        cols = pl.ds(pl.multiple_of(which * half, 128), half)
        return dot(v[:, cols], kd[...], ((0,), (0,)))

    theirs = half_state(1 - x).astype(BF16)
    half_copies = []
    for i in range(CHUNKS):
        half_out[i] = theirs[i * rows : (i + 1) * rows, :]
        copy = remote(half_out.at[i], half_in.at[i], half_send.at[i], half_recv.at[i], across)
        copy.start()
        half_copies.append(copy)
    own_half[...] = half_state(x).reshape(CHUNKS, rows, DK)
    for load in w_loads:
        load.start()
    w_copies = [
        remote(
            w_hbm.at[:, columns(lax.rem(group + j, groups), 1 - core)], w.at[1, j],
            w_send.at[j], w_recv.at[j], partner,
        )
        for j in range(groups)
    ]
    for copy in w_copies:
        copy.start()

    for load in loads[3:]:
        load.wait()
    state[...] = jnp.zeros_like(state)

    def local(b, _):
        part = pl.ds(pl.multiple_of(b * SPAN, SPAN), SPAN)
        r = run[b]
        middle = r[SPAN // 2 : SPAN // 2 + 1, :]
        ending = r[SPAN - 1 : SPAN, :]
        before = ends[pl.ds(b, 1), :]
        qf = q[part, :].astype(F32)
        kf = k[part, :].astype(F32)
        qi = qf * jnp.exp(r)
        qg[part, :] = (qi * jnp.exp(before)).astype(BF16)
        q_intra = (qf * jnp.exp(r - middle)).astype(BF16)
        k_intra = (kf * jnp.exp(middle - r)).astype(BF16)
        k_state = (kf * jnp.exp(ending - r)).astype(BF16)
        vb = v[part, :]
        scores = dot(q_intra, k_intra, ((1,), (1,)))
        weights = jnp.where(tri, scores, 0.0).astype(BF16)
        held = state[...]
        att[part, :] = dot(weights, vb) + dot(qi.astype(BF16), held.astype(BF16), ((1,), (1,)))
        state[...] = held * jnp.exp(ending) + dot(vb, k_state, ((0,), (0,)))
        of = o[part, :].astype(F32)
        act[part, :] = of / (1.0 + jnp.exp(-of)) * gain[...]
        return 0

    early = jnp.where(leads, blocks // 2, blocks)
    lax.fori_loop(0, early, local, 0)

    log_copy.wait()
    mine_log = log_out[0:1, :]
    their_log = log_in[0:1, :]
    first = x == 0
    decay0 = jnp.exp(jnp.where(first, mine_log, their_log))
    decay1 = jnp.exp(jnp.where(first, their_log, mine_log))
    chain_copies = []
    pass_copies = []
    for i in range(CHUNKS):
        half_copies[i].wait_recv()
        chain = remote(
            chain_out.at[i], chain_in.at[i], chain_send.at[i], chain_recv.at[i], onward
        )
        chain_copies.append(chain)
        own = own_half[i]
        other = half_in[i].astype(F32)
        s0 = jnp.where(first, own, other)
        s1 = jnp.where(first, other, own)

        @pl.when(follows)
        def _():
            chain.wait_recv()

        entering = chain_in[i].astype(F32)
        between = decay0 * entering + s0
        chain_out[i] = (decay1 * between + s1).astype(BF16)

        @pl.when(leads)
        def _():
            chain.start()

        pass_out[i] = jnp.where(first, between, entering).astype(BF16)
        carry[x, i] = jnp.where(first, entering, between).astype(BF16)
        passing = remote(
            pass_out.at[i], carry.at[x, i], pass_send.at[i], pass_recv.at[i], across
        )
        passing.start()
        pass_copies.append(passing)
    lax.fori_loop(early, blocks, local, 0)
    for passing in pass_copies:
        passing.wait_recv()
    carried = carry[...].reshape(DV, DK)

    g_copies = []
    for i in range(pieces):
        part = slice(i * TOKENS, (i + 1) * TOKENS)
        a = att[part, :] + dot(qg[part, :], carried, ((1,), (1,)))
        spread = jnp.mean(a * a, axis=-1, keepdims=True)
        gated[0, part, :] = (a * lax.rsqrt(spread + 1e-05) * act[part, :]).astype(BF16)
        copy = remote(
            gated.at[0, part, :], gated.at[1, part, :], g_send.at[i], g_recv.at[i], partner
        )
        copy.start()
        g_copies.append(copy)
    for copy in w_loads:
        copy.wait()
    for copy in w_copies:
        copy.wait_recv()
    y_copies = []
    for i in range(pieces):
        part = slice(i * TOKENS, (i + 1) * TOKENS)
        g_copies[i].wait_recv()
        for j in range(1, groups):
            y_out[j - 1, part, :] = (
                dot(gated[0, part, :], w[0, j]) + dot(gated[1, part, :], w[1, j])
            ).astype(BF16)
            copy = remote(
                y_out.at[j - 1, part, :], y_in.at[j - 1, part, :],
                y_send.at[j - 1, i], y_recv.at[j - 1, i], peers[j - 1],
            )
            copy.start()
            y_copies.append(copy)
    for i in range(pieces):
        part = slice(i * TOKENS, (i + 1) * TOKENS)
        mine[part, :] = dot(gated[0, part, :], w[0, 0]) + dot(gated[1, part, :], w[1, 0])
    for i in range(pieces):
        part = slice(i * TOKENS, (i + 1) * TOKENS)
        total_out = mine[part, :]
        for j in range(1, groups):
            y_copies[i * (groups - 1) + j - 1].wait_recv()
            total_out = total_out + y_in[j - 1, part, :].astype(F32)
        out[part, :] = total_out.astype(BF16)
    for copy in half_copies + pass_copies + w_copies + g_copies + y_copies:
        copy.wait_send()

    @pl.when(leads)
    def _():
        for chain in chain_copies:
            chain.wait_send()


def shards(n_seq, n_head, queries, key_vectors, values, log_gate, out_gate, norm_gain, out_weight):
    length = queries.shape[0]
    width = out_weight.shape[1] // n_head
    groups = n_head // 2
    blocks = length // SPAN
    pieces = length // TOKENS
    half_rows = DV // 2 // CHUNKS
    VM = pltpu.VMEM
    dma = pltpu.SemaphoreType.DMA
    piece_state = (CHUNKS, half_rows, DK)
    scratch = [
        VM((length, DK), BF16), VM((length, DK), BF16), VM((length, DV), BF16),
        VM((length, DK), BF16), VM((length, DV), BF16), VM((1, DV), F32),
        VM((2, groups, DV, width), BF16),
        VM((blocks, SPAN, DK), F32), VM((blocks, DK), F32), VM((length, DK), BF16),
        VM((length, DK), BF16), VM((length, DV), F32), VM((length, DV), F32), VM((DV, DK), F32),
        VM((8, DK), F32), VM((8, DK), F32), VM(piece_state, BF16), VM(piece_state, BF16),
        VM(piece_state, F32), VM(piece_state, BF16), VM(piece_state, BF16),
        VM(piece_state, BF16), VM((2,) + piece_state, BF16),
        VM((2, length, DV), BF16), VM((length, width), F32),
        VM((groups - 1, length, width), BF16), VM((groups - 1, length, width), BF16),
        dma((6,)), dma((groups,)), dma((groups,)), dma((groups,)), dma((2,)),
        dma((CHUNKS,)), dma((CHUNKS,)), dma((CHUNKS,)), dma((CHUNKS,)),
        dma((CHUNKS,)), dma((CHUNKS,)), dma((pieces,)), dma((pieces,)),
        dma((groups - 1, pieces)), dma((groups - 1, pieces)),
    ]
    return pl.pallas_call(
        functools.partial(kernel, n_seq, n_head),
        out_shape=pltpu.VMEM((length, width), BF16),
        in_specs=[pl.BlockSpec(memory_space=pl.ANY)] * 7,
        out_specs=pl.BlockSpec(memory_space=pltpu.VMEM),
        scratch_shapes=scratch,
        compiler_params=pltpu.CompilerParams(
            collective_id=0, has_side_effects=True, vmem_limit_bytes=56 * 2**20
        ),
        name="gated_layer",
    )(queries, key_vectors, values, log_gate, out_gate, norm_gain.reshape(1, DV), out_weight)


def solution(mesh):
    in_specs = (
        P("seq", "head"),
        P("seq", "head"),
        P("seq", "head"),
        P("seq", "head"),
        P("seq", "head"),
        P("head"),
        P("head", None),
    )
    out_specs = P("seq", "head")
    body = functools.partial(shards, mesh.shape["seq"], mesh.shape["head"])
    return jax.shard_map(body, mesh=mesh, in_specs=in_specs, out_specs=out_specs, check_vma=False)
```

```python
import functools

import jax
import jax.numpy as jnp
from jax import lax
from jax.experimental import pallas as pl
from jax.experimental.pallas import tpu as pltpu
from jax.sharding import PartitionSpec as P

DK = 256
DV = 512
SPAN = 64
CHUNKS = 8
TOKENS = 64
DETOUR = 1
HOLD = 6
F32 = jnp.float32
BF16 = jnp.bfloat16
MESH = pl.DeviceIdType.MESH


def dot(a, b, dims=((1,), (0,))):
    return lax.dot_general(a, b, (dims, ((), ())), preferred_element_type=F32)


def kernel(
    n_seq, n_head,
    q_hbm, k_hbm, v_hbm, g_hbm, o_hbm, gain_hbm, w_hbm,
    out,
    q, k, v, g, o, gain, w,
    run, ends, kd, qg, att, act, state,
    log_out, log_in, half_out, half_in, own_half, chain_out, chain_in, pass_out, carry,
    gated, mine, y_out, y_in, decay, near, far,
    load_sem, w_sem, w_send, w_recv, log_sem, half_send, half_recv,
    chain_send, chain_recv, pass_send, pass_recv, g_send, g_recv, y_send, y_recv,
    near_send, near_recv, far_send, far_recv, home_send, home_recv,
):
    length = q.shape[0]
    blocks = length // SPAN
    pieces = length // TOKENS
    groups = n_head // 2
    width = w_hbm.shape[1] // n_head
    half = DK // 2
    rows = half // CHUNKS
    seq = lax.axis_index("seq")
    head = lax.axis_index("head")
    x = lax.rem(seq, 2)
    z = lax.div(seq, 2)
    last = n_seq // 2 - 1
    core = lax.rem(head, 2)
    group = lax.div(head, 2)
    across = {"seq": seq + 1 - 2 * x, "head": head}
    onward = {"seq": lax.rem(seq + 2, n_seq), "head": head}
    back = {"seq": lax.rem(seq + n_seq - 2, n_seq), "head": head}
    leads = z < last
    follows = z > 0
    partner = {"seq": seq, "head": head + 1 - 2 * core}
    peers = [
        {"seq": seq, "head": lax.rem(head + 2 * step, n_head)} for step in range(1, groups)
    ]

    def columns(which_group, which_core):
        return pl.ds(pl.multiple_of((which_group * 2 + which_core) * width, 128), width)

    loads = [
        pltpu.make_async_copy(src, dst, load_sem.at[i])
        for i, (src, dst) in enumerate(
            ((g_hbm, g), (k_hbm, k), (v_hbm, v), (q_hbm, q), (o_hbm, o), (gain_hbm, gain))
        )
    ]
    for load in loads:
        load.start()
    w_loads = [
        pltpu.make_async_copy(
            w_hbm.at[:, columns(lax.rem(group + j, groups), core)], w.at[0, j], w_sem.at[j]
        )
        for j in range(groups)
    ]
    barrier = pltpu.get_barrier_semaphore()

    def greet(friend):
        pl.semaphore_signal(barrier, inc=1, device_id=friend, device_id_type=MESH)

    for friend in [across, partner] + peers:
        greet(friend)
    pl.when(leads)(lambda: greet(onward))
    pl.when(follows)(lambda: greet(back))
    met = 2 + len(peers) + leads.astype(jnp.int32) + follows.astype(jnp.int32)

    def remote(src, dst, send, recv, device):
        return pltpu.make_async_remote_copy(
            src_ref=src, dst_ref=dst, send_sem=send, recv_sem=recv,
            device_id=device, device_id_type=MESH,
        )

    @pl.when(z == 0)
    def _():
        chain_in[...] = jnp.zeros_like(chain_in)

    tri = (
        lax.broadcasted_iota(jnp.int32, (SPAN, SPAN), 0)
        >= lax.broadcasted_iota(jnp.int32, (SPAN, SPAN), 1)
    )
    ones = jnp.where(tri, 1.0, 0.0).astype(BF16)
    loads[0].wait()
    total = jnp.zeros((1, DK), F32)
    endings = []
    for b in range(blocks):
        r = dot(ones, g[b * SPAN : (b + 1) * SPAN, :])
        run[b] = r
        endings.append(r[SPAN - 1 : SPAN, :])
        ends[b : b + 1, :] = total
        total = total + endings[b]
    log_out[...] = jnp.broadcast_to(total, log_out.shape)
    loads[1].wait()
    tail = jnp.zeros((1, DK), F32)
    for b in reversed(range(blocks)):
        part = slice(b * SPAN, (b + 1) * SPAN)
        kd[part, :] = (k[part, :].astype(F32) * jnp.exp((endings[b] - run[b]) + tail)).astype(BF16)
        tail = tail + endings[b]

    pl.semaphore_wait(barrier, met)
    log_copy = remote(log_out, log_in, log_sem.at[0], log_sem.at[1], across)
    log_copy.start()
    loads[2].wait()

    def half_state(which):
        cols = pl.ds(pl.multiple_of(which * half, 128), half)
        return dot(kd[:, cols], v[...], ((0,), (0,)))

    theirs = half_state(1 - x).astype(BF16)
    half_copies = []
    for i in range(CHUNKS):
        half_out[i] = theirs[i * rows : (i + 1) * rows, :]
        copy = remote(half_out.at[i], half_in.at[i], half_send.at[i], half_recv.at[i], across)
        copy.start()
        half_copies.append(copy)
    own_half[...] = half_state(x).reshape(CHUNKS, rows, DV)
    for load in w_loads:
        load.start()
    w_copies = [
        remote(
            w_hbm.at[:, columns(lax.rem(group + j, groups), 1 - core)], w.at[1, j],
            w_send.at[j], w_recv.at[j], partner,
        )
        for j in range(groups)
    ]
    for copy in w_copies:
        copy.start()

    for load in loads[3:]:
        load.wait()
    state[...] = jnp.zeros_like(state)

    def column(row):
        lanes = jnp.broadcast_to(row, (128, DK)).T
        return jnp.concatenate([lanes] * (DV // 128), axis=1)

    def local(b, _):
        part = pl.ds(pl.multiple_of(b * SPAN, SPAN), SPAN)
        r = run[b]
        middle = r[SPAN // 2 : SPAN // 2 + 1, :]
        ending = r[SPAN - 1 : SPAN, :]
        before = ends[pl.ds(b, 1), :]
        qf = q[part, :].astype(F32)
        kf = k[part, :].astype(F32)
        qi = qf * jnp.exp(r)
        qg[part, :] = (qi * jnp.exp(before)).astype(BF16)
        q_intra = (qf * jnp.exp(r - middle)).astype(BF16)
        k_intra = (kf * jnp.exp(middle - r)).astype(BF16)
        k_state = (kf * jnp.exp(ending - r)).astype(BF16)
        vb = v[part, :]
        scores = dot(q_intra, k_intra, ((1,), (1,)))
        weights = jnp.where(tri, scores, 0.0).astype(BF16)
        held = state[...]
        att[part, :] = dot(weights, vb) + dot(qi.astype(BF16), held.astype(BF16))
        state[...] = held * column(jnp.exp(ending)) + dot(k_state, vb, ((0,), (0,)))
        of = o[part, :].astype(F32)
        act[part, :] = of / (1.0 + jnp.exp(-of)) * gain[...]
        return 0

    early = jnp.where(leads, blocks // 2, blocks)
    lax.fori_loop(0, early, local, 0)

    log_copy.wait()
    mine_log = log_out[0:1, :]
    their_log = log_in[0:1, :]
    first = x == 0
    for i, logs in enumerate(
        (jnp.where(first, mine_log, their_log), jnp.where(first, their_log, mine_log))
    ):
        decay[i] = jnp.broadcast_to(jnp.exp(logs), (128, DK)).T

    def decays(i, at):
        lanes = decay[i, pl.ds(pl.multiple_of(x * half + at * rows, rows), rows), :]
        return jnp.concatenate([lanes] * (DV // 128), axis=1)

    chain_copies = []
    pass_copies = []
    for i in range(CHUNKS):
        half_copies[i].wait_recv()
        chain = remote(
            chain_out.at[i], chain_in.at[i], chain_send.at[i], chain_recv.at[i], onward
        )
        chain_copies.append(chain)
        own = own_half[i]
        other = half_in[i].astype(F32)
        s0 = jnp.where(first, own, other)
        s1 = jnp.where(first, other, own)

        @pl.when(follows)
        def _():
            chain.wait_recv()

        entering = chain_in[i].astype(F32)
        between = decays(0, i) * entering + s0
        chain_out[i] = (decays(1, i) * between + s1).astype(BF16)

        @pl.when(leads)
        def _():
            chain.start()

        pass_out[i] = jnp.where(first, between, entering).astype(BF16)
        carry[x, i] = jnp.where(first, entering, between).astype(BF16)
        passing = remote(
            pass_out.at[i], carry.at[x, i], pass_send.at[i], pass_recv.at[i], across
        )
        passing.start()
        pass_copies.append(passing)
    lax.fori_loop(early, blocks, local, 0)
    for passing in pass_copies:
        passing.wait_recv()
    carried = carry[...].reshape(DK, DV)

    g_copies = []
    for i in range(pieces):
        part = slice(i * TOKENS, (i + 1) * TOKENS)
        a = att[part, :] + dot(qg[part, :], carried)
        spread = jnp.mean(a * a, axis=-1, keepdims=True)
        gated[0, part, :] = (a * lax.rsqrt(spread + 1e-05) * act[part, :]).astype(BF16)
        copy = remote(
            gated.at[0, part, :], gated.at[1, part, :], g_send.at[i], g_recv.at[i], partner
        )
        copy.start()
        g_copies.append(copy)
    for copy in w_loads:
        copy.wait()
    for copy in w_copies:
        copy.wait_recv()
    first_pair = z == 0
    direct, nears, fars, homes = {}, {}, {}, {}
    for j in range(groups - 1):
        for i in range(pieces):
            part = slice(i * TOKENS, (i + 1) * TOKENS)
            direct[i, j] = remote(
                y_out.at[j, part, :], y_in.at[j, part, :],
                y_send.at[j, i], y_recv.at[j, i], peers[j],
            )
            if i < DETOUR:
                nears[i, j] = remote(
                    y_out.at[j, part, :], near.at[j, i],
                    near_send.at[j, i], near_recv.at[j, i], back,
                )
                fars[i, j] = remote(
                    near.at[j, i], far.at[j, i], far_send.at[j, i], far_recv.at[j, i], peers[j]
                )
                homes[i, j] = remote(
                    far.at[j, i], y_in.at[j, part, :],
                    home_send.at[j, i], home_recv.at[j, i], onward,
                )
    detours = sorted(nears)
    for i in range(pieces):
        part = slice(i * TOKENS, (i + 1) * TOKENS)
        g_copies[i].wait_recv()
        if i == HOLD:

            @pl.when(leads)
            def _():
                for at in detours:
                    nears[at].wait_recv()
                    fars[at].start()

        for j in range(groups - 1):
            y_out[j, part, :] = (
                dot(gated[0, part, :], w[0, j + 1]) + dot(gated[1, part, :], w[1, j + 1])
            ).astype(BF16)
            if i < DETOUR:
                pl.when(follows)(nears[i, j].start)
                pl.when(first_pair)(direct[i, j].start)
            else:
                direct[i, j].start()
    for i in range(pieces):
        part = slice(i * TOKENS, (i + 1) * TOKENS)
        mine[part, :] = dot(gated[0, part, :], w[0, 0]) + dot(gated[1, part, :], w[1, 0])

    @pl.when(leads)
    def _():
        for at in detours:
            fars[at].wait_recv()
            homes[at].start()

    for i in list(range(DETOUR, pieces)) + list(range(DETOUR)):
        part = slice(i * TOKENS, (i + 1) * TOKENS)
        total_out = mine[part, :]
        for j in range(groups - 1):
            if i < DETOUR:
                pl.when(follows)(homes[i, j].wait_recv)
                pl.when(first_pair)(direct[i, j].wait_recv)
            else:
                direct[i, j].wait_recv()
            total_out = total_out + y_in[j, part, :].astype(F32)
        out[part, :] = total_out.astype(BF16)

    @pl.when(follows)
    def _():
        for at in detours:
            nears[at].wait_send()

    @pl.when(first_pair)
    def _():
        for at in detours:
            direct[at].wait_send()

    @pl.when(leads)
    def _():
        for at in detours:
            fars[at].wait_send()
            homes[at].wait_send()

    y_copies = [direct[at] for at in direct if at not in nears]
    for copy in half_copies + pass_copies + w_copies + g_copies + y_copies:
        copy.wait_send()

    @pl.when(leads)
    def _():
        for chain in chain_copies:
            chain.wait_send()


def shards(n_seq, n_head, queries, key_vectors, values, log_gate, out_gate, norm_gain, out_weight):
    length = queries.shape[0]
    width = out_weight.shape[1] // n_head
    groups = n_head // 2
    blocks = length // SPAN
    pieces = length // TOKENS
    half_rows = DK // 2 // CHUNKS
    VM = pltpu.VMEM
    dma = pltpu.SemaphoreType.DMA
    piece_state = (CHUNKS, half_rows, DV)
    scratch = [
        VM((length, DK), BF16), VM((length, DK), BF16), VM((length, DV), BF16),
        VM((length, DK), BF16), VM((length, DV), BF16), VM((1, DV), F32),
        VM((2, groups, DV, width), BF16),
        VM((blocks, SPAN, DK), F32), VM((blocks, DK), F32), VM((length, DK), BF16),
        VM((length, DK), BF16), VM((length, DV), F32), VM((length, DV), F32), VM((DK, DV), F32),
        VM((8, DK), F32), VM((8, DK), F32), VM(piece_state, BF16), VM(piece_state, BF16),
        VM(piece_state, F32), VM(piece_state, BF16), VM(piece_state, BF16),
        VM(piece_state, BF16), VM((2,) + piece_state, BF16),
        VM((2, length, DV), BF16), VM((length, width), F32),
        VM((groups - 1, length, width), BF16), VM((groups - 1, length, width), BF16),
        VM((2, DK, 128), F32),
        VM((groups - 1, DETOUR, TOKENS, width), BF16), VM((groups - 1, DETOUR, TOKENS, width), BF16),
        dma((6,)), dma((groups,)), dma((groups,)), dma((groups,)), dma((2,)),
        dma((CHUNKS,)), dma((CHUNKS,)), dma((CHUNKS,)), dma((CHUNKS,)),
        dma((CHUNKS,)), dma((CHUNKS,)), dma((pieces,)), dma((pieces,)),
        dma((groups - 1, pieces)), dma((groups - 1, pieces)),
    ] + [dma((groups - 1, DETOUR))] * 6 + [
    ]
    return pl.pallas_call(
        functools.partial(kernel, n_seq, n_head),
        out_shape=pltpu.VMEM((length, width), BF16),
        in_specs=[pl.BlockSpec(memory_space=pl.ANY)] * 7,
        out_specs=pl.BlockSpec(memory_space=pltpu.VMEM),
        scratch_shapes=scratch,
        compiler_params=pltpu.CompilerParams(
            collective_id=0, has_side_effects=True, vmem_limit_bytes=56 * 2**20
        ),
        name="gated_layer",
    )(queries, key_vectors, values, log_gate, out_gate, norm_gain.reshape(1, DV), out_weight)


def solution(mesh):
    in_specs = (
        P("seq", "head"),
        P("seq", "head"),
        P("seq", "head"),
        P("seq", "head"),
        P("seq", "head"),
        P("head"),
        P("head", None),
    )
    out_specs = P("seq", "head")
    body = functools.partial(shards, mesh.shape["seq"], mesh.shape["head"])
    return jax.shard_map(body, mesh=mesh, in_specs=in_specs, out_specs=out_specs, check_vma=False)
```
